16 devices in a mesh: ep: 16 (over z, y, x, core).
Axes of the slice: x: 2, y: 2, z: 2, core: 2. Of those that a mesh axis runs over, the one named last changes fastest.
Arguments:
- x_in: bfloat16 [16384, 2048], P('ep')
- route_idx: int32 [16384, 8], P('ep')
- gate_w: bfloat16 [16384, 8], P('ep')
- dy_in: bfloat16 [16384, 2048], P('ep')
- w_gate: bfloat16 [16, 2048, 768], P('ep')
- w_up: bfloat16 [16, 2048, 768], P('ep')
- w_down: bfloat16 [16, 768, 2048], P('ep')
- hot_gate: bfloat16 [2048, 768], replicated
- hot_up: bfloat16 [2048, 768], replicated
- hot_down: bfloat16 [768, 2048], replicated
Outputs:
- output 1: bfloat16 [16384, 2048], P('ep')
- output 2: bfloat16 [16384, 2048], P('ep')
- output 3: float32 [16, 2048, 768], P('ep')
- output 4: float32 [16, 2048, 768], P('ep')
- output 5: float32 [16, 768, 2048], P('ep')
- output 6: float32 [2048, 768], P(None, 'ep')
- output 7: float32 [2048, 768], P(None, 'ep')
- output 8: float32 [768, 2048], P('ep')
All inputs are finite; a program needn't handle non-finite values.
Results may differ from the reference program's by a relative error of at most 0.0107547.
Values are sent between devices in bfloat16 or wider.
A program may use at most 1 GiB of HBM per device.

```python
import jax
import jax.numpy as jnp
from jax import lax

N_DEV = 16
TOK_DEV = 1024
D_MODEL = 2048
D_FF = 768
TOP_K = 8

SLOT_CAP = min(TOK_DEV, 2 * TOK_DEV * TOP_K // N_DEV)
HOT_CAP = 3 * TOK_DEV // 4
TOTAL = N_DEV * TOK_DEV


def draw_routes(rng_key):
    heavy_key, weight_key, hot_key, pick_key, order_key, shift_key = jax.random.split(rng_key, 6)
    expert_ids = jnp.arange(N_DEV, dtype=jnp.int32)
    heavy = jax.random.randint(heavy_key, (N_DEV,), 0, N_DEV)
    is_heavy = expert_ids[None, :] == heavy[:, None]
    weight = jnp.where(is_heavy, 0, jax.random.randint(weight_key, (N_DEV, N_DEV), 1, 9))
    hot_count = jax.random.randint(hot_key, (N_DEV,), HOT_CAP // 4, HOT_CAP + 1)
    hot_count = jnp.where(expert_ids == jax.random.randint(pick_key, (), 0, N_DEV), HOT_CAP, hot_count)
    rest = TOK_DEV * TOP_K - hot_count - SLOT_CAP
    base = jnp.minimum((rest[:, None] * weight) // jnp.sum(weight, axis=1, keepdims=True), SLOT_CAP)
    room = jnp.where(is_heavy, 0, SLOT_CAP - base)
    deficit = rest - jnp.sum(base, axis=1)
    before = jnp.cumsum(room, axis=1) - room
    extra = jnp.minimum(jnp.maximum(deficit[:, None] - before, 0), room)
    load = base + extra + jnp.where(is_heavy, SLOT_CAP, 0)
    bounds = jnp.cumsum(jnp.concatenate([load, hot_count[:, None]], axis=1), axis=1)
    positions = jnp.arange(TOK_DEV * TOP_K, dtype=jnp.int32)
    ordered = jax.vmap(lambda bound_row: jnp.searchsorted(bound_row, positions, side='right'))(bounds)
    grid = ordered.reshape(N_DEV, TOP_K, TOK_DEV).transpose(0, 2, 1)
    token_order = jax.vmap(lambda sub_key: jax.random.permutation(sub_key, TOK_DEV))(jax.random.split(order_key, N_DEV))
    grid = jnp.take_along_axis(grid, token_order[:, :, None], axis=1)
    shift = jax.random.randint(shift_key, (N_DEV, TOK_DEV, 1), 0, TOP_K)
    col_index = (jnp.arange(TOP_K, dtype=jnp.int32)[None, None, :] + shift) % TOP_K
    grid = jnp.take_along_axis(grid, col_index, axis=2)
    return grid.reshape(TOTAL, TOP_K).astype(jnp.int32)


def setup_inputs(seed: int = 0) -> dict:
    sub_keys = jax.random.split(jax.random.key(seed), 10)
    in_scale = D_MODEL ** -0.5
    hid_scale = D_FF ** -0.5
    x_in = jax.random.normal(sub_keys[0], (TOTAL, D_MODEL), jnp.float32).astype(jnp.bfloat16)
    route_idx = draw_routes(sub_keys[1])
    gate_w = jax.random.uniform(sub_keys[2], (TOTAL, TOP_K), jnp.float32, 0.5, 1.5).astype(jnp.bfloat16)
    dy_in = jax.random.normal(sub_keys[3], (TOTAL, D_MODEL), jnp.float32).astype(jnp.bfloat16)
    w_gate = (jax.random.normal(sub_keys[4], (N_DEV, D_MODEL, D_FF), jnp.float32) * in_scale).astype(jnp.bfloat16)
    w_up = (jax.random.normal(sub_keys[5], (N_DEV, D_MODEL, D_FF), jnp.float32) * in_scale).astype(jnp.bfloat16)
    w_down = (jax.random.normal(sub_keys[6], (N_DEV, D_FF, D_MODEL), jnp.float32) * hid_scale).astype(jnp.bfloat16)
    hot_gate = (jax.random.normal(sub_keys[7], (D_MODEL, D_FF), jnp.float32) * in_scale).astype(jnp.bfloat16)
    hot_up = (jax.random.normal(sub_keys[8], (D_MODEL, D_FF), jnp.float32) * in_scale).astype(jnp.bfloat16)
    hot_down = (jax.random.normal(sub_keys[9], (D_FF, D_MODEL), jnp.float32) * hid_scale).astype(jnp.bfloat16)
    return {'x_in': x_in, 'route_idx': route_idx, 'gate_w': gate_w, 'dy_in': dy_in, 'w_gate': w_gate, 'w_up': w_up, 'w_down': w_down, 'hot_gate': hot_gate, 'hot_up': hot_up, 'hot_down': hot_down}


def silu_parts(pre_gate):
    sig_val = jax.nn.sigmoid(pre_gate)
    return pre_gate * sig_val, sig_val * (1.0 + pre_gate * (1.0 - sig_val))


def expert_pass(x_rows, d_rows, gate_mat, up_mat, down_mat):
    u_val = jnp.dot(x_rows, gate_mat, preferred_element_type=jnp.float32)
    v_val = jnp.dot(x_rows, up_mat, preferred_element_type=jnp.float32)
    silu_val, silu_grad = silu_parts(u_val)
    hidden = (silu_val * v_val).astype(jnp.bfloat16)
    result = jnp.dot(hidden, down_mat, preferred_element_type=jnp.float32).astype(jnp.bfloat16)
    grad_hidden = jnp.dot(d_rows, down_mat.T, preferred_element_type=jnp.float32).astype(jnp.bfloat16).astype(jnp.float32)
    grad_u = (grad_hidden * v_val * silu_grad).astype(jnp.bfloat16)
    grad_v = (grad_hidden * silu_val).astype(jnp.bfloat16)
    grad_x = (jnp.dot(grad_u, gate_mat.T, preferred_element_type=jnp.float32) + jnp.dot(grad_v, up_mat.T, preferred_element_type=jnp.float32)).astype(jnp.bfloat16)
    grad_gate = jnp.dot(x_rows.T, grad_u, preferred_element_type=jnp.float32)
    grad_up = jnp.dot(x_rows.T, grad_v, preferred_element_type=jnp.float32)
    grad_down = jnp.dot(hidden.T, d_rows, preferred_element_type=jnp.float32)
    return result, grad_x, (grad_gate, grad_up, grad_down)


def reference(x_in, route_idx, gate_w, dy_in, w_gate, w_up, w_down, hot_gate, hot_up, hot_down):
    flat_ids = route_idx.reshape(-1)
    n_assign = flat_ids.shape[0]
    order = jnp.argsort(flat_ids, stable=True)
    starts = jnp.searchsorted(flat_ids[order], jnp.arange(N_DEV + 2, dtype=jnp.int32), side='left')
    gate_flat = gate_w.reshape(-1)

    def take_block(first, last, max_rows):
        position = first + jnp.arange(max_rows, dtype=jnp.int32)
        assign = jnp.where(position < last, order[jnp.minimum(position, n_assign - 1)], n_assign)
        token = assign // TOP_K
        x_rows = jnp.take(x_in, token, axis=0, mode='fill', fill_value=0)
        gate_rows = jnp.take(gate_flat, assign, mode='fill', fill_value=0).astype(jnp.float32)
        dy_rows = jnp.take(dy_in, token, axis=0, mode='fill', fill_value=0).astype(jnp.float32)
        d_rows = (gate_rows[:, None] * dy_rows).astype(jnp.bfloat16)
        return token, gate_rows, x_rows, d_rows

    def add_block(sums, token, gate_rows, result, grad_x):
        y_sum, dx_sum = sums
        y_sum = y_sum.at[token].add(gate_rows[:, None] * result.astype(jnp.float32), mode='drop')
        dx_sum = dx_sum.at[token].add(grad_x.astype(jnp.float32), mode='drop')
        return y_sum, dx_sum

    def regular_step(sums, expert_args):
        gate_mat, up_mat, down_mat, first, last = expert_args
        token, gate_rows, x_rows, d_rows = take_block(first, last, N_DEV * SLOT_CAP)
        result, grad_x, grads = expert_pass(x_rows, d_rows, gate_mat, up_mat, down_mat)
        return add_block(sums, token, gate_rows, result, grad_x), grads

    zero_sum = jnp.zeros((TOTAL, D_MODEL), jnp.float32)
    sums, (dw_gate, dw_up, dw_down) = lax.scan(regular_step, (zero_sum, zero_sum), (w_gate, w_up, w_down, starts[:N_DEV], starts[1:N_DEV + 1]))
    token, gate_rows, x_rows, d_rows = take_block(starts[N_DEV], starts[N_DEV + 1], N_DEV * HOT_CAP)
    result, grad_x, (dhot_gate, dhot_up, dhot_down) = expert_pass(x_rows, d_rows, hot_gate, hot_up, hot_down)
    y_sum, dx_sum = add_block(sums, token, gate_rows, result, grad_x)
    return (y_sum.astype(jnp.bfloat16), dx_sum.astype(jnp.bfloat16), dw_gate, dw_up, dw_down, dhot_gate, dhot_up, dhot_down)
```

```python
import jax
import jax.numpy as jnp
from jax import lax
from jax.sharding import PartitionSpec as P


CONTRACT_LAST = (((1,), (1,)), ((), ()))
CONTRACT_FIRST = (((0,), (0,)), ((), ()))


def dot_f32(lhs, rhs, dims=(((1,), (0,)), ((), ()))):
    return lax.dot_general(lhs, rhs, dims, preferred_element_type=jnp.float32)


def forward(x_rows, gate, chosen, gate_mat, up_mat, down_mat):
    u_val = dot_f32(x_rows, gate_mat)
    v_val = dot_f32(x_rows, up_mat)
    hidden = jnp.where(chosen, (u_val * jax.nn.sigmoid(u_val) * v_val).astype(jnp.bfloat16), 0)
    result = dot_f32(hidden, down_mat).astype(jnp.bfloat16).astype(jnp.float32)
    return gate * result, (u_val, v_val, hidden)


def backward(saved, dy_rows, gate, chosen, gate_mat, up_mat, down_mat):
    u_val, v_val, _ = saved
    scaled = (gate * dy_rows.astype(jnp.float32)).astype(jnp.bfloat16)
    grad_hidden = dot_f32(scaled, down_mat, CONTRACT_LAST).astype(jnp.bfloat16).astype(jnp.float32)
    sig_val = jax.nn.sigmoid(u_val)
    silu_grad = sig_val * (1.0 + u_val * (1.0 - sig_val))
    grad_u = jnp.where(chosen, (grad_hidden * v_val * silu_grad).astype(jnp.bfloat16), 0)
    grad_v = jnp.where(chosen, (grad_hidden * (u_val * sig_val)).astype(jnp.bfloat16), 0)
    grad_x = (dot_f32(grad_u, gate_mat, CONTRACT_LAST) + dot_f32(grad_v, up_mat, CONTRACT_LAST)).astype(jnp.bfloat16)
    return grad_x.astype(jnp.float32), (scaled, grad_u, grad_v)


def weight_grads(x_rows, saved, grads):
    scaled, grad_u, grad_v = grads
    return (dot_f32(x_rows, grad_u, CONTRACT_FIRST), dot_f32(x_rows, grad_v, CONTRACT_FIRST), dot_f32(saved[2], scaled, CONTRACT_FIRST))


def solution(mesh):
    n_dev = mesh.shape['ep']
    half = n_dev // 2
    planes = [list(range(half)), list(range(half, n_dev))]
    across = [(i, (i + half) % n_dev) for i in range(n_dev)]

    def local_step(x_loc, route_loc, gate_loc, dy_loc, w_gate, w_up, w_down, hot_gate, hot_up, hot_down):
        me = lax.axis_index('ep')
        own = (w_gate[0], w_up[0], w_down[0])
        other = tuple(lax.ppermute(w, 'ep', across) for w in own)

        def plane_gather(rows):
            return lax.all_gather(rows, 'ep', axis=0, tiled=True, axis_index_groups=planes)

        def column(route, gate, expert):
            hit = route == expert
            value = jnp.sum(jnp.where(hit, gate.astype(jnp.float32), 0.0), axis=1, keepdims=True)
            return value, jnp.any(hit, axis=1, keepdims=True)

        route_all, gate_all = plane_gather(route_loc), plane_gather(gate_loc)
        x_all = plane_gather(x_loc)
        dy_all = plane_gather(dy_loc)
        hot_col = column(route_loc, gate_loc, n_dev)
        own_col = column(route_all, gate_all, me)
        other_col = column(route_all, gate_all, lax.rem(me + half, n_dev))

        y_hot, saved_hot = forward(x_loc, *hot_col, hot_gate, hot_up, hot_down)
        dx_hot, grads_hot = backward(saved_hot, dy_loc, *hot_col, hot_gate, hot_up, hot_down)
        dhot = weight_grads(x_loc, saved_hot, grads_hot)

        y_own, saved_own = forward(x_all, *own_col, *own)
        y_other, saved_other = forward(x_all, *other_col, *other)
        y_sum = lax.psum_scatter(y_own + y_other, 'ep', scatter_dimension=0, tiled=True, axis_index_groups=planes)
        dx_other, grads_other = backward(saved_other, dy_all, *other_col, *other)
        dx_own, grads_own = backward(saved_own, dy_all, *own_col, *own)
        dx_sum = lax.psum_scatter(dx_own + dx_other, 'ep', scatter_dimension=0, tiled=True, axis_index_groups=planes)
        dw_other = weight_grads(x_all, saved_other, grads_other)
        dw_back = tuple(lax.ppermute(w, 'ep', across) for w in dw_other)
        dw_own = weight_grads(x_all, saved_own, grads_own)
        dw = tuple((a + b)[None] for a, b in zip(dw_own, dw_back))
        dhot = (lax.psum_scatter(dhot[0], 'ep', scatter_dimension=1, tiled=True),
                lax.psum_scatter(dhot[1], 'ep', scatter_dimension=1, tiled=True),
                lax.psum_scatter(dhot[2], 'ep', scatter_dimension=0, tiled=True))
        return ((y_sum + y_hot).astype(jnp.bfloat16), (dx_sum + dx_hot).astype(jnp.bfloat16), *dw, *dhot)

    row_spec = P('ep', None)
    expert_spec = P('ep', None, None)
    whole_spec = P(None, None)
    return jax.shard_map(local_step, mesh=mesh, in_specs=(row_spec, row_spec, row_spec, row_spec, expert_spec, expert_spec, expert_spec, whole_spec, whole_spec, whole_spec), out_specs=(row_spec, row_spec, expert_spec, expert_spec, expert_spec, P(None, 'ep'), P(None, 'ep'), P('ep', None)), check_vma=False)
```

```python
import jax
import jax.numpy as jnp
from jax import lax
from jax.sharding import PartitionSpec as P


CONTRACT_LAST = (((1,), (1,)), ((), ()))
CONTRACT_FIRST = (((0,), (0,)), ((), ()))
CORE, AXIS_X, AXIS_Y, AXIS_Z = 1, 2, 4, 8


def dot_f32(lhs, rhs, dims=(((1,), (0,)), ((), ()))):
    return lax.dot_general(lhs, rhs, dims, preferred_element_type=jnp.float32)


def swap(rows, bit):
    return lax.ppermute(rows, 'ep', [(i, i ^ bit) for i in range(16)])


def after(value, *others):
    return lax.optimization_barrier((value,) + others)[0]


def spread(rows):
    half = rows.shape[0] // 2
    from_x, from_y = swap(rows, AXIS_X), swap(rows, AXIS_Y)
    top, bottom = swap(from_y[:half], AXIS_X), swap(from_x[half:], AXIS_Y)
    return jnp.concatenate([rows, from_x, from_y, top, bottom], axis=0), (top, bottom)


def collect(mine, got):
    tok_rows, half = mine.shape[0] // 4, mine.shape[1] // 2
    grids = tuple(t.reshape(2, 2, tok_rows, 2 * half) for t in (mine, got))
    left, right = slice(0, half), slice(half, 2 * half)

    def part(pair, y_side, x_side, cols):
        return pair[0][y_side, x_side, :, cols] + pair[1][y_side, x_side, :, cols]

    send_left = part(grids, slice(0, 2), 1, left)
    send_right = part(grids, 1, slice(0, 2), right)
    pair = lax.optimization_barrier((*grids, send_left, send_right))[:2]
    got_left = swap(send_left, AXIS_X)
    got_right = swap(send_right, AXIS_Y)
    relay_left = part(pair, 1, 0, left) + got_left[1]
    late = lax.optimization_barrier((*pair, got_right, relay_left))
    relay_right = part(late, 0, 1, right) + late[2][1]
    last_left = swap(relay_left, AXIS_Y)
    last_right = swap(relay_right, AXIS_X)

    def finish(local, *wait):
        last = lax.optimization_barrier((*pair, got_left, got_right, relay_left, relay_right) + wait)
        sum_left = part(last, 0, 0, left) + last[2][0] + last_left
        sum_right = part(last, 0, 0, right) + last[3][0] + last_right
        return (jnp.concatenate([sum_left, sum_right], axis=1) + local).astype(jnp.bfloat16)

    return finish, (send_left, send_right)


def column(route, gate, expert):
    hit = route == expert
    value = jnp.sum(jnp.where(hit, gate.astype(jnp.float32), 0.0), axis=1, keepdims=True)
    return value, jnp.any(hit, axis=1, keepdims=True)


def hidden_of(x_rows, chosen, pair_mat):
    pair = dot_f32(x_rows, pair_mat)
    u_val, v_val = jnp.split(pair, 2, axis=1)
    hidden = jnp.where(chosen, (u_val * jax.nn.sigmoid(u_val) * v_val).astype(jnp.bfloat16), 0)
    return pair, hidden


def result_of(hidden, gate, down_mat):
    return gate * dot_f32(hidden, down_mat).astype(jnp.bfloat16).astype(jnp.float32)


def scale(gate, dy_rows):
    return (gate * dy_rows.astype(jnp.float32)).astype(jnp.bfloat16)


def hidden_grads(pair, scaled, chosen, down_mat):
    u_val, v_val = jnp.split(pair, 2, axis=1)
    grad_hidden = dot_f32(scaled, down_mat, CONTRACT_LAST).astype(jnp.bfloat16).astype(jnp.float32)
    sig_val = jax.nn.sigmoid(u_val)
    silu_grad = sig_val * (1.0 + u_val * (1.0 - sig_val))
    grad_u = jnp.where(chosen, (grad_hidden * v_val * silu_grad).astype(jnp.bfloat16), 0)
    grad_v = jnp.where(chosen, (grad_hidden * (u_val * sig_val)).astype(jnp.bfloat16), 0)
    return jnp.concatenate([grad_u, grad_v], axis=1)


def input_grad(grad_pair, pair_mat):
    return dot_f32(grad_pair, pair_mat, CONTRACT_LAST).astype(jnp.bfloat16).astype(jnp.float32)


def solution(mesh):
    n_dev = mesh.shape['ep']
    half_dev = n_dev // 2
    planes = [list(range(half_dev)), list(range(half_dev, n_dev))]

    def local_step(x_loc, route_loc, gate_loc, dy_loc, w_gate, w_up, w_down, hot_gate, hot_up, hot_down):
        me = lax.axis_index('ep')
        place = lax.rem(me, half_dev)
        far = tuple(swap(w[0], AXIS_Z) for w in (w_gate, w_up, w_down))
        far = (jnp.concatenate(far[:2], axis=1), far[2])
        own = (jnp.concatenate([w_gate[0], w_up[0]], axis=1), w_down[0])
        hot = jnp.concatenate([hot_gate, hot_up], axis=1)
        x_same, x_relay = spread(x_loc)
        table = after(jnp.concatenate([route_loc.astype(jnp.bfloat16), gate_loc], axis=1), *x_relay)
        table = lax.all_gather(table, 'ep', axis=0, axis_index_groups=planes)
        dy_same, _ = spread(after(dy_loc, table))

        def pick(bits):
            rows = jnp.concatenate([lax.dynamic_index_in_dim(table, jnp.bitwise_xor(place, b), 0, keepdims=False) for b in bits], axis=0)
            return rows[:, :8].astype(jnp.int32), rows[:, 8:]

        picked = [pick((0, 2, 4, 6)), pick((1, 3, 5, 7))]
        routes, gates = [p[0] for p in picked], [p[1] for p in picked]
        gate_hot, chosen_hot = column(route_loc, gate_loc, n_dev)
        pair_hot, hidden_hot = hidden_of(x_loc, chosen_hot, hot)
        y_hot = result_of(hidden_hot, gate_hot, hot_down)
        scaled_hot = scale(gate_hot, dy_loc)
        grad_hot = hidden_grads(pair_hot, scaled_hot, chosen_hot, hot_down)
        dx_hot = input_grad(grad_hot, hot)

        dhot = [dot_f32(a, b, CONTRACT_FIRST) for a, b in ((grad_hot[:, :768], x_loc), (grad_hot[:, 768:], x_loc), (hidden_hot, scaled_hot))]
        x_same = after(x_same, y_hot, dx_hot, *dhot)
        xs = (x_same, swap(x_same, CORE))
        weights = {'own': own, 'far': far}
        cols = {'own': [column(r, g, me) for r, g in zip(routes, gates)],
                'far': [column(r, g, jnp.bitwise_xor(me, half_dev)) for r, g in zip(routes, gates)]}
        saved, y_part = {}, {}

        def forward(name, s, *wait):
            saved[name, s] = hidden_of(after(xs[s], *wait), cols[name][s][1], weights[name][0])

        def y_of(s):
            y_part[s] = sum(result_of(saved[name, s][1], cols[name][s][0], weights[name][1]) for name in ('own', 'far'))

        forward('own', 0)
        forward('own', 1, saved['own', 0][1])
        forward('far', 1, saved['own', 1][1])
        y_of(1)
        forward('far', 0, y_part[1])
        y_of(0)
        finish_y, y_sent = collect(y_part[0], swap(y_part[1], CORE))

        dys = (dy_same, swap(dy_same, CORE))
        grads, dx_part, flow = {}, {}, {}

        def hidden_back(name, s, *wait):
            flow[s] = after(dys[s], *wait)
            grads[name, s] = hidden_grads(saved[name, s][0], scale(cols[name][s][0], flow[s]), cols[name][s][1], weights[name][1])

        def dx_of(s):
            dx_part[s] = sum(input_grad(grads[name, s], weights[name][0]) for name in ('own', 'far'))

        def down_grad(name, *wait):
            return sum(dot_f32(saved[name, s][1], scale(cols[name][s][0], after(dys[s], *wait)), CONTRACT_FIRST) for s in (0, 1))

        def pair_grad(name, *wait):
            return sum(dot_f32(after(xs[s], *wait), grads[name, s], CONTRACT_FIRST) for s in (0, 1))

        hidden_back('far', 1, *y_sent)
        hidden_back('far', 0, *y_sent)
        far_pair = pair_grad('far', grads['far', 0], grads['far', 1])
        back_pair = swap(far_pair, AXIS_Z)
        hidden_back('own', 1, far_pair)
        dx_of(1)
        hidden_back('own', 0, dx_part[1])
        dx_of(0)
        finish_dx, dx_sent = collect(dx_part[0], swap(dx_part[1], CORE))
        y_out = finish_y(y_hot, *dx_sent)
        dx_out = finish_dx(dx_hot)
        far_down = down_grad('far', *dx_sent)
        back_down = swap(far_down, AXIS_Z)
        dhot = lax.optimization_barrier((*dhot, dy_same))[:3]
        dhot = [lax.psum_scatter(d, 'ep', scatter_dimension=0, tiled=True) for d in dhot]
        own_down = down_grad('own', far_down)
        own_pair = pair_grad('own', own_down)
        dw_down = (own_down + back_down)[None]
        dw_gate, dw_up = jnp.split((own_pair + back_pair)[None], 2, axis=2)
        return (y_out, dx_out, dw_gate, dw_up, dw_down, dhot[0].T, dhot[1].T, dhot[2])

    row_spec = P('ep', None)
    expert_spec = P('ep', None, None)
    whole_spec = P(None, None)
    return jax.shard_map(local_step, mesh=mesh, in_specs=(row_spec, row_spec, row_spec, row_spec, expert_spec, expert_spec, expert_spec, whole_spec, whole_spec, whole_spec), out_specs=(row_spec, row_spec, expert_spec, expert_spec, expert_spec, P(None, 'ep'), P(None, 'ep'), P('ep', None)), check_vma=False)
```
